32 devices in a mesh: outer: 4 (over y, x), inner: 8 (over z, core).
Axes of the slice: x: 2, y: 2, z: 4, core: 2. Of those that a mesh axis runs over, the one named last changes fastest.
Arguments:
- queries: bfloat16 [8192, 16, 128], P(('outer', 'inner')), may hold values from -6 to 6
- key_rows: bfloat16 [8192, 16, 128], P(('outer', 'inner')), may hold values from -6 to 6
- value_rows: bfloat16 [8192, 16, 128], P(('outer', 'inner')), may hold values from -6 to 6
- key_scale: bfloat16 [8192, 16], P(('outer', 'inner')), may hold values from 0.5 to 2
- value_scale: bfloat16 [8192, 16], P(('outer', 'inner')), may hold values from 0.5 to 2
- cluster_label: int32 [16, 8192, 1], P(None, ('outer', 'inner')), may hold values from 0 to 127; in each aligned block of 256 rows (0 to 255, 256 to 511, ..., all dimensions but the last counted through in order) at most 4 rows name the same one
Outputs:
- attended: bfloat16 [8192, 16, 128], P(('outer', 'inner'))
The draws below stay inside these ranges and needn't reach their ends.
Inputs may be any that keep to these rules, and one draw needn't show every extreme that they name: `cluster_label`: among the 256 rows of one device for one head, no label occurs more than 4 times, and some label occurs exactly 4 times.
All inputs are finite; a program needn't handle non-finite values.
Results may differ from the reference program's by a relative error of at most 0.0033.
Values may be sent and summed in bfloat16 or wider, within the bound.
A program may use at most 64 MiB of HBM per device.

```python
import math
import jax
import jax.numpy as jnp
import numpy as np
from jax import lax

HEADS = 16
HEAD = 128
COARSE = 16
FINE = 8
TOK_DEV = 256
CLUSTERS = 128
CAP = 4
TOKENS = 8192
N_OUTER = 4
N_INNER = 8


def draw_vectors(key, fold_tag):
    drawn = jax.random.normal(jax.random.fold_in(key, fold_tag), (TOKENS, HEADS, HEAD), jnp.float32)
    return jnp.clip(drawn, -6.0, 6.0).astype(jnp.bfloat16)


def draw_queries(key, part):
    return draw_vectors(key, 11)


def draw_key_rows(key, part):
    return draw_vectors(key, 13)


def levels(own_key, dims, pieces, low, high):
    gain = 1.0
    for axis_at, blocks in pieces:
        steps = jax.random.uniform(jax.random.fold_in(jax.random.fold_in(own_key, 6), axis_at), (blocks,), jnp.float32, low / len(pieces), high / len(pieces))
        gain = gain * jnp.repeat(jnp.exp(steps), dims[axis_at] // blocks).reshape((-1,) + (1,) * (len(dims) - 1 - axis_at))
    return gain


def routed_block(rng, own, number, rows, amount, top, reach, lean):
    sequence = jax.random.permutation(rng, amount)
    heavy_load, ordinary = shares(amount, rows * top, reach, lean, True), shares(amount, rows * top, reach, lean, False)
    places = jnp.arange(amount)

    def named(sizes, offset_by):
        used = int((sizes > 0).sum())
        fixed = max(1, used // 4)
        shifted = fixed + (places - fixed + offset_by * (used - fixed)) % max(1, amount - fixed)
        return jnp.zeros((amount,), jnp.int32).at[sequence[jnp.where(places < fixed, places, shifted)]].set(jnp.asarray(sizes, jnp.int32))

    sizes = jnp.where(number % 4 == 0, named(heavy_load, number // 4), named(ordinary, number - number // 4 - 1))
    mixed = jax.random.permutation(jax.random.fold_in(own, 3), amount)
    donor, receiver = mixed[0:amount // 2 * 2:2], mixed[1:amount // 2 * 2:2]
    margin = jnp.minimum(sizes[donor] - 1, reach - sizes[receiver]) // 2
    margin = jnp.where((donor == sequence[0]) | (receiver == sequence[0]) | (sizes[receiver] == 0), 0, jnp.maximum(margin, 0))
    shifted = jax.random.randint(jax.random.fold_in(own, 4), (amount // 2,), 0, 1 << 20) % (margin + 1)
    sizes = sizes.at[donor].add(-shifted).at[receiver].add(shifted)
    items = jnp.searchsorted(jnp.cumsum(sizes), jnp.arange(rows * top), side="right").astype(jnp.int32)
    table = items.reshape(top, rows).T
    table = table[jax.random.permutation(jax.random.fold_in(own, 1), rows)]
    offset_by = jax.random.randint(jax.random.fold_in(own, 2), (rows, 1), 0, top)
    return jnp.take_along_axis(table, (jnp.arange(top)[None, :] + offset_by) % top, axis=1)


def shares(count, total, most, slope, full):
    loads = [(1 << 20) // math.isqrt(rank ** slope) + 1 for rank in range(1, count + 1)]
    largest = most if full else min(most, max(-(-total // count), total * loads[0] // sum(loads)))
    least = 1 if total - largest >= count - 1 else 0
    holding, spare = [largest] + [least] * (count - 1), total - largest - least * (count - 1)
    while spare > 0:
        free = [i for i in range(1, count) if holding[i] < largest] or [i for i in range(1, count) if holding[i] < most]
        mass, budget = sum([loads[i] for i in free]), spare
        for i in free:
            addition = min(most - holding[i], max(1, budget * loads[i] // mass), spare)
            holding[i] = holding[i] + addition
            spare = spare - addition
    return np.array(holding)


def noise(rng, dims, scale, reach, split=(), kind=jnp.bfloat16):
    loudness = levels(rng, dims, split, -0.22, 0.18) if split else 1.0
    values = jax.random.normal(rng, dims, jnp.float32) * scale * loudness
    return jnp.minimum(jnp.maximum(values, -reach), reach).astype(kind)


def setup_inputs(seed: int = 0) -> dict:
    arg_keys = jax.random.split(jax.random.key(seed), 7)
    queries = draw_queries(jax.random.fold_in(arg_keys[6], 71), 0)
    key_rows = draw_key_rows(jax.random.fold_in(arg_keys[6], 71), 0)
    value_rows = noise(arg_keys[2], (TOKENS, HEADS, HEAD), 1.0, 6.0, ((0, 32),))
    key_scale = jnp.clip(jnp.exp(math.log(2.0) - 1.3862944 * jax.random.uniform(arg_keys[3], (TOKENS, HEADS), jnp.float32) ** levels(arg_keys[3], (TOKENS, HEADS), ((0, 32),), -0.2, 0.2)), 0.5, 2.0).astype(jnp.bfloat16)
    value_scale = jnp.clip(jnp.exp(math.log(2.0) - 1.3862944 * jax.random.uniform(arg_keys[4], (TOKENS, HEADS), jnp.float32) ** levels(arg_keys[4], (TOKENS, HEADS), ((0, 32),), -0.2, 0.2)), 0.5, 2.0).astype(jnp.bfloat16)
    cluster_label_keys = jax.random.split(jax.random.fold_in(arg_keys[5], 1), HEADS * TOKENS // TOK_DEV)
    cluster_label_turns = jax.random.permutation(jax.random.fold_in(arg_keys[5], 3), HEADS * TOKENS // TOK_DEV)
    cluster_label = jax.vmap(lambda own, number: routed_block(jax.random.fold_in(arg_keys[5], 2), own, number, TOK_DEV, CLUSTERS, 1, CAP, 2))(cluster_label_keys, cluster_label_turns).reshape((HEADS, TOKENS, 1))
    return dict(queries=queries, key_rows=key_rows, value_rows=value_rows, key_scale=key_scale, value_scale=value_scale, cluster_label=cluster_label)


def attend(query_block, key_block, value_block, key_factor, value_factor, position):
    factor = query_block.shape[-1] ** -0.5
    scores = jnp.dot(query_block, key_block.T, preferred_element_type=jnp.float32)
    scores = scores * (key_factor.astype(jnp.float32) * factor)[None, :]
    visible = (position[None, :] >= 0) & (position[None, :] <= position[:, None])
    highest = jnp.max(jnp.where(visible, scores, jnp.float32(-1e30)), axis=1, keepdims=True)
    unnormed = jnp.where(visible, jnp.exp(scores - highest), jnp.float32(0.0))
    denominator = jnp.sum(unnormed, axis=1)
    weights = (unnormed * value_factor.astype(jnp.float32)[None, :]).astype(jnp.bfloat16)
    numerator = jnp.dot(weights, value_block, preferred_element_type=jnp.float32)
    safe = jnp.where(denominator > 0, denominator, jnp.float32(1.0))
    return (numerator / safe[:, None]).astype(jnp.bfloat16)


def reference(queries, key_rows, value_rows, key_scale, value_scale, cluster_label):
    cluster_count = COARSE * FINE
    window = N_OUTER * N_INNER * CAP
    token_count = queries.shape[0]
    width = queries.shape[2]

    def per_head(inputs):
        query_head, key_head, value_head, key_factor, value_factor, labels = inputs
        order = jnp.argsort(labels, stable=True).astype(jnp.int32)
        counts = jnp.zeros((cluster_count,), jnp.int32).at[labels].add(1)
        starts = jnp.cumsum(counts) - counts

        def per_cluster(which):
            offset = jnp.arange(window, dtype=jnp.int32)
            inside = offset < counts[which]
            token = order[jnp.minimum(starts[which] + offset, token_count - 1)]
            position = jnp.where(inside, token, -1).astype(jnp.int32)
            result = attend(query_head[token], key_head[token], value_head[token],
                            key_factor[token], value_factor[token], position)
            target = jnp.where(inside, token, token_count).astype(jnp.int32)
            return result, target

        results, targets = lax.map(per_cluster, jnp.arange(cluster_count, dtype=jnp.int32))
        empty = jnp.zeros((token_count, width), jnp.bfloat16)
        return empty.at[targets.reshape(-1)].set(results.reshape(-1, width), mode="drop")

    stacked = lax.map(per_head, (jnp.swapaxes(queries, 0, 1), jnp.swapaxes(key_rows, 0, 1),
                                 jnp.swapaxes(value_rows, 0, 1), key_scale.T, value_scale.T,
                                 cluster_label[:, :, 0]))
    return jnp.swapaxes(stacked, 0, 1)
```

```python
import jax
import jax.numpy as jnp
from jax import lax
from jax.experimental import pallas as pl
from jax.experimental.pallas import tpu as pltpu
from jax.sharding import PartitionSpec as P

COARSE = 16
FINE = 8


def attend(query_block, key_block, value_block, key_factor, value_factor, position):
    factor = query_block.shape[-1] ** (-0.5)
    scores = jnp.dot(query_block, key_block.T, preferred_element_type=jnp.float32)
    scores = scores * (key_factor.astype(jnp.float32) * factor)[None, :]
    visible = (position[None, :] >= 0) & (position[None, :] <= position[:, None])
    highest = jnp.max(jnp.where(visible, scores, jnp.float32(-1e30)), axis=1, keepdims=True)
    unnormed = jnp.where(visible, jnp.exp(scores - highest), jnp.float32(0.0))
    denominator = jnp.sum(unnormed, axis=1)
    weights = (unnormed * value_factor.astype(jnp.float32)[None, :]).astype(jnp.bfloat16)
    numerator = jnp.dot(weights, value_block, preferred_element_type=jnp.float32)
    safe = jnp.where(denominator > 0, denominator, jnp.float32(1.0))
    return (numerator / safe[:, None]).astype(jnp.bfloat16)


def attend_items(query_part, key_part, value_part, key_factor, value_factor, position):
    leading = query_part.shape[:3]
    slots = query_part.shape[3]
    width = query_part.shape[4]
    total = leading[0] * leading[1] * leading[2]

    def single(inputs):
        return attend(*inputs)

    results = lax.map(
        single,
        (
            query_part.reshape(total, slots, width),
            key_part.reshape(total, slots, width),
            value_part.reshape(total, slots, width),
            key_factor.reshape(total, slots),
            value_factor.reshape(total, slots),
            position.reshape(total, slots),
        ),
    )
    return results.reshape(leading + (slots, width))


def shards(queries, key_rows, value_rows, key_scale, value_scale, cluster_label):
    outer_count = lax.axis_size("outer")
    inner_count = lax.axis_size("inner")
    tok_rows, heads, width = queries.shape
    cluster_count = COARSE * FINE
    capacity = max(2, 2 * tok_rows // cluster_count)
    labels = cluster_label[:, :, 0].T
    member = (
        labels[:, :, None] == jnp.arange(cluster_count, dtype=jnp.int32)[None, None, :]
    ).astype(jnp.int32)
    rank = jnp.sum(jnp.cumsum(member, axis=0) * member, axis=2) - 1
    slot = (labels * heads + jnp.arange(heads, dtype=jnp.int32)[None, :]) * capacity + rank
    flat = slot.reshape(-1)
    total = cluster_count * heads * capacity
    item_count = cluster_count * heads // (outer_count * inner_count)
    layout = (outer_count, inner_count, item_count, capacity)
    source = (
        jnp.full((total,), -1, jnp.int32)
        .at[flat]
        .set(jnp.arange(tok_rows * heads, dtype=jnp.int32))
    )
    filled_slot = source >= 0
    source_row = jnp.maximum(source, 0)

    def place(array):
        rows = array.reshape((tok_rows * heads,) + array.shape[2:])
        picked = rows[source_row]
        mask = filled_slot.reshape((total,) + (1,) * (picked.ndim - 1))
        kept = jnp.where(mask, picked, jnp.zeros((), array.dtype))
        return kept.reshape(layout + array.shape[2:])

    device = lax.axis_index("outer") * inner_count + lax.axis_index("inner")
    position_rows = jnp.where(filled_slot, device * tok_rows + source_row // heads, -1).reshape(
        layout
    )
    outgoing = (
        place(queries),
        place(key_rows),
        place(value_rows),
        place(key_scale),
        place(value_scale),
        position_rows,
    )
    arrived = (
        lax.all_to_all(
            lax.all_to_all(outgoing[0], "outer", split_axis=0, concat_axis=3, tiled=True),
            "inner",
            split_axis=1,
            concat_axis=3,
            tiled=True,
        ),
        lax.all_to_all(
            lax.all_to_all(outgoing[1], "outer", split_axis=0, concat_axis=3, tiled=True),
            "inner",
            split_axis=1,
            concat_axis=3,
            tiled=True,
        ),
        lax.all_to_all(
            lax.all_to_all(outgoing[2], "outer", split_axis=0, concat_axis=3, tiled=True),
            "inner",
            split_axis=1,
            concat_axis=3,
            tiled=True,
        ),
        lax.all_to_all(
            lax.all_to_all(outgoing[3], "outer", split_axis=0, concat_axis=3, tiled=True),
            "inner",
            split_axis=1,
            concat_axis=3,
            tiled=True,
        ),
        lax.all_to_all(
            lax.all_to_all(outgoing[4], "outer", split_axis=0, concat_axis=3, tiled=True),
            "inner",
            split_axis=1,
            concat_axis=3,
            tiled=True,
        ),
        lax.all_to_all(
            lax.all_to_all(outgoing[5], "outer", split_axis=0, concat_axis=3, tiled=True),
            "inner",
            split_axis=1,
            concat_axis=3,
            tiled=True,
        ),
    )
    answered = attend_items(*arrived)
    returned = lax.all_to_all(
        lax.all_to_all(answered, "inner", split_axis=3, concat_axis=1, tiled=True),
        "outer",
        split_axis=3,
        concat_axis=0,
        tiled=True,
    )
    rows_back = returned.reshape(total, width)
    return rows_back[flat].reshape(tok_rows, heads, width)

AUX = 4


def exchange_kernel(
    chips, half, tok, slots, k_in, v_in, q_in, ks_ref, vs_ref, label_ref, out_ref,
    raw, kv, qt, aux, recv, recv_q, recv_aux, ans, back, kp, vp, xp, qp, op, kb, vb, scales,
    vis_ref, f_scale, load_sem, asend, arecv, send_sem, recv_sem, fasend, farecv, fsend, frecv,
    qsend, qrecv, bsend, brecv,
):
    f32, bf16 = jnp.float32, jnp.bfloat16
    width = kv.shape[2]
    inner = lax.axis_index("inner")
    chip = lax.axis_index("outer") * half + inner // 2
    core = inner % 2
    mine = 2 * chip + core
    partner = {"outer": lax.axis_index("outer"), "inner": inner + 1 - 2 * core}
    far_bit = half // 2
    crossing = [d for d in range(1, chips) if d & far_bit]
    staying = [d for d in range(1, chips) if not d & far_bit]

    def at(other):
        return {"outer": other // half, "inner": (other % half) * 2 + core}

    def copy(src, dst, s1, s2, where):
        return pltpu.make_async_remote_copy(
            src_ref=src, dst_ref=dst, send_sem=s1, recv_sem=s2,
            device_id=where, device_id_type=pl.DeviceIdType.MESH,
        )

    barrier = pltpu.get_barrier_semaphore()

    @pl.loop(1, chips)
    def _(d):
        pl.semaphore_signal(
            barrier, inc=1, device_id=at((chip + d) % chips),
            device_id_type=pl.DeviceIdType.MESH,
        )

    pl.semaphore_signal(
        barrier, inc=1, device_id=partner, device_id_type=pl.DeviceIdType.MESH
    )

    def load(which, source):
        return pltpu.make_async_copy(source, raw.at[which], load_sem.at[which])

    load(0, k_in).start()
    load(1, v_in).start()
    load(2, q_in).start()

    clusters = COARSE * FINE
    capacity = slots // clusters
    earlier = (
        lax.broadcasted_iota(jnp.int32, (tok, tok), 0)
        < lax.broadcasted_iota(jnp.int32, (tok, tok), 1)
    ).astype(f32).astype(bf16)
    f_scale[0] = ks_ref[...].astype(f32)
    f_scale[1] = vs_ref[...].astype(f32)
    aux_row = lax.broadcasted_iota(jnp.int32, (AUX, tok), 0)

    @pl.loop(0, chips)
    def _(h):
        label = label_ref[h]
        member = jnp.where(
            lax.broadcasted_iota(jnp.int32, (clusters, tok), 0) == label, f32(1.0), f32(0.0)
        )
        before = jnp.dot(member.astype(bf16), earlier, preferred_element_type=f32)
        rank = jnp.sum(before * member, axis=0, keepdims=True)
        first_two = jnp.where(
            aux_row == 0, f_scale[0, pl.ds(h, 1), :], f_scale[1, pl.ds(h, 1), :]
        )
        last_two = jnp.where(aux_row == 2, (label * capacity).astype(f32), rank)
        aux[h] = jnp.where(aux_row < 2, first_two, last_two).astype(bf16)

    load(0, k_in).wait()
    kv[:, :tok, :] = jnp.swapaxes(raw[0], 0, 1)
    load(1, v_in).wait()
    kv[:, tok:, :] = jnp.swapaxes(raw[1], 0, 1)
    pl.semaphore_wait(barrier, chips)

    def out_aux(d):
        other = chip ^ d
        return copy(aux.at[other], recv_aux.at[mine], asend.at[d], arecv.at[d], at(other))

    def outgoing(d):
        other = chip ^ d
        return copy(kv.at[other], recv.at[mine], send_sem.at[d], recv_sem.at[d], at(other))

    def outgoing_query(d):
        other = chip ^ d
        return copy(qt.at[other], recv_q.at[chip], qsend.at[d], qrecv.at[d], at(other))

    def own_aux():
        return copy(aux.at[chip], recv_aux.at[mine], fasend.at[0], farecv.at[0], partner)

    def own_forward():
        return copy(kv.at[chip], recv.at[mine], fsend.at[0], frecv.at[0], partner)

    def forward_aux(d):
        row = 2 * (chip ^ d) + core
        return copy(recv_aux.at[row], recv_aux.at[row], fasend.at[d], farecv.at[d], partner)

    def forward(d):
        row = 2 * (chip ^ d) + core
        return copy(recv.at[row], recv.at[row], fsend.at[d], frecv.at[d], partner)

    for d in crossing + staying:
        out_aux(d).start()
    own_aux().start()
    for i, d in enumerate(crossing):
        outgoing(d).start()
        if i < len(staying):
            outgoing(staying[i]).start()
    own_forward().start()
    load(2, q_in).wait()
    qt[...] = jnp.swapaxes(raw[2], 0, 1)

    lane = lax.broadcasted_iota(jnp.int32, (tok, width), 1)
    low = (lane < width // 2).astype(f32).astype(bf16)
    high = (lane >= width // 2).astype(f32).astype(bf16)

    for d in staying + crossing:
        outgoing_query(d).start()

    recv[mine] = kv[chip]
    recv_aux[mine] = aux[chip]
    recv_q[chip] = qt[chip]

    key_at = lax.broadcasted_iota(jnp.int32, vis_ref.shape, 1)
    query_at = lax.broadcasted_iota(jnp.int32, vis_ref.shape, 0)
    turn = query_at // 8
    away = turn % far_bit + (turn // far_bit) % (chips // 2 // far_bit) * (2 * far_bit)
    away = away + turn // (chips // 2) * far_bit
    key_order = (key_at // 8) * 4 + key_at % 4
    query_order = (2 * (away ^ chip) + core) * 4 + query_at % 4
    same = (key_at // 4) % 2 == (query_at // 4) % 2
    vis_ref[...] = jnp.where(same & (key_order <= query_order), f32(1.0), f32(0.0))
    turns = [0] + staying + crossing

    def aux_of(row):
        return recv_aux[row].astype(f32)

    def hits(extra):
        slot = (extra[2:3] + extra[3:4]).astype(jnp.int32)
        return lax.broadcasted_iota(jnp.int32, (slots, tok), 0) == slot

    def one_hot(hit):
        return jnp.where(hit, f32(1.0), f32(0.0)).astype(bf16)

    def place(row):
        extra = aux_of(row)
        hit = hits(extra)
        one = one_hot(hit)
        by_key = jnp.where(hit, extra[0:1], f32(0.0)).astype(bf16)
        by_value = jnp.where(hit, extra[1:2], f32(0.0)).astype(bf16)
        kp[row] = jnp.dot(one, recv[row, pl.ds(0, tok)], preferred_element_type=f32)
        vp[row] = jnp.dot(one, recv[row, pl.ds(tok, tok)], preferred_element_type=f32)
        xp[row] = jnp.dot(by_key, low, preferred_element_type=f32) + jnp.dot(
            by_value, high, preferred_element_type=f32
        )

    def place_query(turn, other):
        qp[turn] = jnp.dot(
            one_hot(hits(aux_of(2 * other + core))), recv_q[other], preferred_element_type=f32
        )

    place(mine)
    own_aux().wait_recv()
    own_forward().wait_recv()
    place(2 * chip + 1 - core)

    def of_turn(t):
        side = chips // 2
        low_part = t % far_bit + (t // far_bit) % (side // far_bit) * (2 * far_bit)
        return low_part + t // side * far_bit

    @pl.loop(1, chips)
    def _(t):
        d = of_turn(t)
        out_aux(d).wait_recv()
        forward_aux(d).start()
        outgoing(d).wait_recv()
        forward(d).start()
        place(2 * (chip ^ d) + core)

        @pl.when(t > 1)
        def _():
            before = of_turn(t - 1)
            forward_aux(before).wait_recv()
            forward(before).wait_recv()
            place(2 * (chip ^ before) + 1 - core)

    last = turns[-1]
    forward_aux(last).wait_recv()
    forward(last).wait_recv()
    place(2 * (chip ^ last) + 1 - core)

    sel_lane = lax.broadcasted_iota(jnp.int32, (16, width), 1)
    sel_row = lax.broadcasted_iota(jnp.int32, (16, width), 0)
    select = (sel_lane == jnp.where(sel_row < 8, 0, width // 2)).astype(f32).astype(bf16)
    factor = width ** (-0.5)
    keys_here = vis_ref.shape[1]
    chunk_rows = CHUNK * 8
    nt = (((1,), (1,)), ((), ()))

    def rows_of(t):
        return pl.ds(pl.multiple_of(t * 8, 8), 8)

    @pl.loop(0, slots // 8 // UNROLL)
    def _(at_group):
        for u in range(UNROLL):
            t = at_group * UNROLL + u
            rows = rows_of(t)
            kb[t] = kp[:, rows, :].reshape(keys_here, width).astype(bf16)
            vb[t] = vp[:, rows, :].reshape(keys_here, width).astype(bf16)
            extra = xp[:, rows, :].reshape(keys_here, width).astype(bf16)
            scales[t] = lax.dot_general(select, extra, nt, preferred_element_type=f32)

    def attend_groups(base, groups):
        here = pl.ds(base, CHUNK)
        allowed = vis_ref[pl.ds(base * 8, chunk_rows), :]
        scale = [scales[t] for t in groups]
        query = [qp[here, rows_of(t), :].reshape(chunk_rows, width).astype(bf16) for t in groups]
        scores = [
            lax.dot_general(q, kb[t], nt, preferred_element_type=f32)
            for q, t in zip(query, groups)
        ]
        visible = [allowed * c[0:1] > 0 for c in scale]
        scores = [
            jnp.where(ok, s * (c[0:1] * factor), f32(-1e30))
            for ok, s, c in zip(visible, scores, scale)
        ]
        highest = [jnp.max(s, axis=1, keepdims=True) for s in scores]
        unnormed = [
            jnp.where(ok, jnp.exp(s - m), f32(0.0))
            for ok, s, m in zip(visible, scores, highest)
        ]
        weights = [(e * c[8:9]).astype(bf16) for e, c in zip(unnormed, scale)]
        numerator = [
            jnp.dot(w, vb[t], preferred_element_type=f32) for w, t in zip(weights, groups)
        ]
        denominator = [jnp.sum(e, axis=1, keepdims=True) for e in unnormed]
        safe = [jnp.where(n > 0, n, f32(1.0)) for n in denominator]
        result = [(n / d).astype(bf16).astype(f32) for n, d in zip(numerator, safe)]
        for r, t in zip(result, groups):
            op[here, rows_of(t), :] = r.reshape(CHUNK, 8, width)

    eye = (
        lax.broadcasted_iota(jnp.int32, (tok, tok), 0)
        == lax.broadcasted_iota(jnp.int32, (tok, tok), 1)
    ).astype(f32).astype(bf16)

    def answer(turn, other):
        columns = lax.dot_general(
            eye, recv_aux[2 * other + core], (((1,), (1,)), ((), ())), preferred_element_type=f32,
        )
        slot = (columns[:, 2:3] + columns[:, 3:4]).astype(jnp.int32)
        hit = lax.broadcasted_iota(jnp.int32, (tok, slots), 1) == slot
        return jnp.dot(
            one_hot(hit), op[turn].astype(bf16), preferred_element_type=f32
        ).astype(bf16)

    def reply(d):
        other = chip ^ d
        return copy(ans.at[other], back.at[chip], bsend.at[d], brecv.at[d], at(other))

    place_query(0, chip)
    for part in range(chips // CHUNK):
        first_turn = part * CHUNK
        start = max(first_turn, 1)

        @pl.loop(start, first_turn + CHUNK)
        def _(t):
            d = of_turn(t)
            outgoing_query(d).wait_recv()
            place_query(t, chip ^ d)

        @pl.loop(0, slots // 8 // UNROLL)
        def _(at_group):
            attend_groups(first_turn, [at_group * UNROLL + u for u in range(UNROLL)])

        @pl.loop(start, first_turn + CHUNK)
        def _(t):
            other = chip ^ of_turn(t)
            ans[other] = answer(t, other)

            @pl.when(t > start)
            def _():
                reply(of_turn(t - 1)).start()

        reply(of_turn(first_turn + CHUNK - 1)).start()

    back[chip] = answer(0, chip)
    own_forward().wait_send()
    own_aux().wait_send()

    @pl.loop(1, chips)
    def _(d):
        out_aux(d).wait_send()
        outgoing(d).wait_send()
        outgoing_query(d).wait_send()
        forward_aux(d).wait_send()
        forward(d).wait_send()
        reply(d).wait()

    out_ref[...] = jnp.swapaxes(back[...], 0, 1)


def by_head(queries, key_rows, value_rows, key_scale, value_scale, cluster_label):
    tok, heads, width = queries.shape
    half = lax.axis_size("inner") // 2
    chips = lax.axis_size("outer") * half
    clusters = COARSE * FINE
    slots = clusters * max(2, 2 * tok // clusters)
    vm = pl.BlockSpec(memory_space=pltpu.VMEM)
    anywhere = pl.BlockSpec(memory_space=pl.ANY)
    dma = pltpu.SemaphoreType.DMA
    f32, bf16 = jnp.float32, jnp.bfloat16
    return pl.pallas_call(
        lambda *refs: exchange_kernel(chips, half, tok, slots, *refs),
        out_shape=jax.ShapeDtypeStruct((tok, heads, width), bf16),
        in_specs=[anywhere] * 3 + [vm] * 3,
        out_specs=vm,
        scratch_shapes=[
            pltpu.VMEM((3, tok, heads, width), bf16),
            pltpu.VMEM((heads, 2 * tok, width), bf16),
            pltpu.VMEM((heads, tok, width), bf16),
            pltpu.VMEM((heads, AUX, tok), bf16),
            pltpu.VMEM((2 * chips, 2 * tok, width), bf16),
            pltpu.VMEM((chips, tok, width), bf16),
            pltpu.VMEM((2 * chips, AUX, tok), bf16),
            pltpu.VMEM((chips, tok, width), bf16),
            pltpu.VMEM((chips, tok, width), bf16),
            pltpu.VMEM((2 * chips, slots, width), f32),
            pltpu.VMEM((2 * chips, slots, width), f32),
            pltpu.VMEM((2 * chips, slots, width), f32),
            pltpu.VMEM((chips, slots, width), f32),
            pltpu.VMEM((chips, slots, width), f32),
            pltpu.VMEM((slots // 8, 16 * chips, width), bf16),
            pltpu.VMEM((slots // 8, 16 * chips, width), bf16),
            pltpu.VMEM((slots // 8, 16, 16 * chips), f32),
            pltpu.VMEM((8 * chips, 16 * chips), f32),
            pltpu.VMEM((2, heads, tok), f32),
            dma((3,)),
        ]
        + [dma((chips,))] * 12,
        compiler_params=pltpu.CompilerParams(
            collective_id=0, has_side_effects=True, vmem_limit_bytes=63 * 1024 * 1024
        ),
        name="clustered",
    )(
        key_rows, value_rows, queries, key_scale.T, value_scale.T, cluster_label.swapaxes(1, 2)
    )


UNROLL = 16
CHUNK = 4


def route(queries, key_rows, value_rows, key_scale, value_scale, cluster_label):
    tok, heads, width = queries.shape
    devices = lax.axis_size("outer") * lax.axis_size("inner")
    even = lax.axis_size("inner") % 2 == 0 and tok == 2 * width
    even = even and heads & (heads - 1) == 0 and heads % CHUNK == 0
    if devices == 2 * heads and even and 2 * tok == 4 * COARSE * FINE:
        return by_head(queries, key_rows, value_rows, key_scale, value_scale, cluster_label)
    return shards(queries, key_rows, value_rows, key_scale, value_scale, cluster_label)


def solution(mesh):
    placed = (
        P(("outer", "inner"), None, None),
        P(("outer", "inner"), None, None),
        P(("outer", "inner"), None, None),
        P(("outer", "inner"), None),
        P(("outer", "inner"), None),
        P(None, ("outer", "inner"), None),
    )
    return jax.shard_map(
        route,
        mesh=mesh,
        in_specs=placed,
        out_specs=P(("outer", "inner"), None, None),
        check_vma=False,
    )
```

```python
import jax
import jax.numpy as jnp
from jax import lax
from jax.experimental import pallas as pl
from jax.experimental.pallas import tpu as pltpu
from jax.sharding import PartitionSpec as P

COARSE = 16
FINE = 8


def attend(query_block, key_block, value_block, key_factor, value_factor, position):
    factor = query_block.shape[-1] ** (-0.5)
    scores = jnp.dot(query_block, key_block.T, preferred_element_type=jnp.float32)
    scores = scores * (key_factor.astype(jnp.float32) * factor)[None, :]
    visible = (position[None, :] >= 0) & (position[None, :] <= position[:, None])
    highest = jnp.max(jnp.where(visible, scores, jnp.float32(-1e30)), axis=1, keepdims=True)
    unnormed = jnp.where(visible, jnp.exp(scores - highest), jnp.float32(0.0))
    denominator = jnp.sum(unnormed, axis=1)
    weights = (unnormed * value_factor.astype(jnp.float32)[None, :]).astype(jnp.bfloat16)
    numerator = jnp.dot(weights, value_block, preferred_element_type=jnp.float32)
    safe = jnp.where(denominator > 0, denominator, jnp.float32(1.0))
    return (numerator / safe[:, None]).astype(jnp.bfloat16)


def attend_items(query_part, key_part, value_part, key_factor, value_factor, position):
    leading = query_part.shape[:3]
    slots = query_part.shape[3]
    width = query_part.shape[4]
    total = leading[0] * leading[1] * leading[2]

    def single(inputs):
        return attend(*inputs)

    results = lax.map(
        single,
        (
            query_part.reshape(total, slots, width),
            key_part.reshape(total, slots, width),
            value_part.reshape(total, slots, width),
            key_factor.reshape(total, slots),
            value_factor.reshape(total, slots),
            position.reshape(total, slots),
        ),
    )
    return results.reshape(leading + (slots, width))


def shards(queries, key_rows, value_rows, key_scale, value_scale, cluster_label):
    outer_count = lax.axis_size("outer")
    inner_count = lax.axis_size("inner")
    tok_rows, heads, width = queries.shape
    cluster_count = COARSE * FINE
    capacity = max(2, 2 * tok_rows // cluster_count)
    labels = cluster_label[:, :, 0].T
    member = (
        labels[:, :, None] == jnp.arange(cluster_count, dtype=jnp.int32)[None, None, :]
    ).astype(jnp.int32)
    rank = jnp.sum(jnp.cumsum(member, axis=0) * member, axis=2) - 1
    slot = (labels * heads + jnp.arange(heads, dtype=jnp.int32)[None, :]) * capacity + rank
    flat = slot.reshape(-1)
    total = cluster_count * heads * capacity
    item_count = cluster_count * heads // (outer_count * inner_count)
    layout = (outer_count, inner_count, item_count, capacity)
    source = (
        jnp.full((total,), -1, jnp.int32)
        .at[flat]
        .set(jnp.arange(tok_rows * heads, dtype=jnp.int32))
    )
    filled_slot = source >= 0
    source_row = jnp.maximum(source, 0)

    def place(array):
        rows = array.reshape((tok_rows * heads,) + array.shape[2:])
        picked = rows[source_row]
        mask = filled_slot.reshape((total,) + (1,) * (picked.ndim - 1))
        kept = jnp.where(mask, picked, jnp.zeros((), array.dtype))
        return kept.reshape(layout + array.shape[2:])

    device = lax.axis_index("outer") * inner_count + lax.axis_index("inner")
    position_rows = jnp.where(filled_slot, device * tok_rows + source_row // heads, -1).reshape(
        layout
    )
    outgoing = (
        place(queries),
        place(key_rows),
        place(value_rows),
        place(key_scale),
        place(value_scale),
        position_rows,
    )
    arrived = (
        lax.all_to_all(
            lax.all_to_all(outgoing[0], "outer", split_axis=0, concat_axis=3, tiled=True),
            "inner",
            split_axis=1,
            concat_axis=3,
            tiled=True,
        ),
        lax.all_to_all(
            lax.all_to_all(outgoing[1], "outer", split_axis=0, concat_axis=3, tiled=True),
            "inner",
            split_axis=1,
            concat_axis=3,
            tiled=True,
        ),
        lax.all_to_all(
            lax.all_to_all(outgoing[2], "outer", split_axis=0, concat_axis=3, tiled=True),
            "inner",
            split_axis=1,
            concat_axis=3,
            tiled=True,
        ),
        lax.all_to_all(
            lax.all_to_all(outgoing[3], "outer", split_axis=0, concat_axis=3, tiled=True),
            "inner",
            split_axis=1,
            concat_axis=3,
            tiled=True,
        ),
        lax.all_to_all(
            lax.all_to_all(outgoing[4], "outer", split_axis=0, concat_axis=3, tiled=True),
            "inner",
            split_axis=1,
            concat_axis=3,
            tiled=True,
        ),
        lax.all_to_all(
            lax.all_to_all(outgoing[5], "outer", split_axis=0, concat_axis=3, tiled=True),
            "inner",
            split_axis=1,
            concat_axis=3,
            tiled=True,
        ),
    )
    answered = attend_items(*arrived)
    returned = lax.all_to_all(
        lax.all_to_all(answered, "inner", split_axis=3, concat_axis=1, tiled=True),
        "outer",
        split_axis=3,
        concat_axis=0,
        tiled=True,
    )
    rows_back = returned.reshape(total, width)
    return rows_back[flat].reshape(tok_rows, heads, width)

AUX = 4


def exchange_kernel(
    chips, half, tok, slots, k_in, v_in, q_in, ks_ref, vs_ref, label_ref, out_ref,
    raw, kv, qt, aux, recv, recv_q, recv_aux, ans, back, kp, vp, xp, qp, op, kb, vb, scales,
    vis_ref, f_scale, load_sem, asend, arecv, send_sem, recv_sem, fasend, farecv, fsend, frecv,
    qsend, qrecv, bsend, brecv,
):
    f32, bf16 = jnp.float32, jnp.bfloat16
    width = kv.shape[2]
    inner = lax.axis_index("inner")
    chip = lax.axis_index("outer") * half + inner // 2
    core = inner % 2
    mine = 2 * chip + core
    partner = {"outer": lax.axis_index("outer"), "inner": inner + 1 - 2 * core}
    far_bit = half // 2
    crossing = [d for d in range(1, chips) if d & far_bit]
    staying = [d for d in range(1, chips) if not d & far_bit]

    def at(other):
        return {"outer": other // half, "inner": (other % half) * 2 + core}

    def copy(src, dst, s1, s2, where):
        return pltpu.make_async_remote_copy(
            src_ref=src, dst_ref=dst, send_sem=s1, recv_sem=s2,
            device_id=where, device_id_type=pl.DeviceIdType.MESH,
        )

    barrier = pltpu.get_barrier_semaphore()

    @pl.loop(1, chips)
    def _(d):
        pl.semaphore_signal(
            barrier, inc=1, device_id=at((chip + d) % chips),
            device_id_type=pl.DeviceIdType.MESH,
        )

    pl.semaphore_signal(
        barrier, inc=1, device_id=partner, device_id_type=pl.DeviceIdType.MESH
    )

    def load(which, source):
        return pltpu.make_async_copy(source, raw.at[which], load_sem.at[which])

    load(0, k_in).start()
    load(1, v_in).start()
    load(2, q_in).start()

    clusters = COARSE * FINE
    capacity = slots // clusters
    earlier = (
        lax.broadcasted_iota(jnp.int32, (tok, tok), 0)
        < lax.broadcasted_iota(jnp.int32, (tok, tok), 1)
    ).astype(f32).astype(bf16)
    f_scale[0] = ks_ref[...].astype(f32)
    f_scale[1] = vs_ref[...].astype(f32)
    aux_row = lax.broadcasted_iota(jnp.int32, (AUX, tok), 0)

    @pl.loop(0, chips)
    def _(h):
        label = label_ref[h]
        member = jnp.where(
            lax.broadcasted_iota(jnp.int32, (clusters, tok), 0) == label, f32(1.0), f32(0.0)
        )
        before = jnp.dot(member.astype(bf16), earlier, preferred_element_type=f32)
        rank = jnp.sum(before * member, axis=0, keepdims=True)
        first_two = jnp.where(
            aux_row == 0, f_scale[0, pl.ds(h, 1), :], f_scale[1, pl.ds(h, 1), :]
        )
        last_two = jnp.where(aux_row == 2, (label * capacity).astype(f32), rank)
        aux[h] = jnp.where(aux_row < 2, first_two, last_two).astype(bf16)

    load(0, k_in).wait()
    kv[:, :tok, :] = jnp.swapaxes(raw[0], 0, 1)
    load(1, v_in).wait()
    kv[:, tok:, :] = jnp.swapaxes(raw[1], 0, 1)
    pl.semaphore_wait(barrier, chips)

    def out_aux(d):
        other = chip ^ d
        return copy(aux.at[other], recv_aux.at[mine], asend.at[d], arecv.at[d], at(other))

    def outgoing(d):
        other = chip ^ d
        return copy(kv.at[other], recv.at[mine], send_sem.at[d], recv_sem.at[d], at(other))

    def outgoing_query(d):
        other = chip ^ d
        return copy(qt.at[other], recv_q.at[chip], qsend.at[d], qrecv.at[d], at(other))

    def own_aux():
        return copy(aux.at[chip], recv_aux.at[mine], fasend.at[0], farecv.at[0], partner)

    def own_forward():
        return copy(kv.at[chip], recv.at[mine], fsend.at[0], frecv.at[0], partner)

    def forward_aux(d):
        row = 2 * (chip ^ d) + core
        return copy(recv_aux.at[row], recv_aux.at[row], fasend.at[d], farecv.at[d], partner)

    def forward(d):
        row = 2 * (chip ^ d) + core
        return copy(recv.at[row], recv.at[row], fsend.at[d], frecv.at[d], partner)

    for d in crossing + staying:
        out_aux(d).start()
    own_aux().start()
    for d in range(1, chips):
        outgoing(d).start()
    own_forward().start()
    load(2, q_in).wait()
    qt[...] = jnp.swapaxes(raw[2], 0, 1)

    lane = lax.broadcasted_iota(jnp.int32, (tok, width), 1)
    low = (lane < width // 2).astype(f32).astype(bf16)
    high = (lane >= width // 2).astype(f32).astype(bf16)

    for d in range(1, chips):
        outgoing_query(d).start()

    recv[mine] = kv[chip]
    recv_aux[mine] = aux[chip]
    recv_q[chip] = qt[chip]

    key_at = lax.broadcasted_iota(jnp.int32, vis_ref.shape, 1)
    query_at = lax.broadcasted_iota(jnp.int32, vis_ref.shape, 0)
    turn = query_at // 8
    away = turn
    key_order = (key_at // 8) * 4 + key_at % 4
    query_order = (2 * (away ^ chip) + core) * 4 + query_at % 4
    same = (key_at // 4) % 2 == (query_at // 4) % 2
    vis_ref[...] = jnp.where(same & (key_order <= query_order), f32(1.0), f32(0.0))
    turns = list(range(chips))

    def aux_of(row):
        return recv_aux[row].astype(f32)

    def hits(extra):
        slot = (extra[2:3] + extra[3:4]).astype(jnp.int32)
        return lax.broadcasted_iota(jnp.int32, (slots, tok), 0) == slot

    def one_hot(hit):
        return jnp.where(hit, f32(1.0), f32(0.0)).astype(bf16)

    def place(row):
        extra = aux_of(row)
        hit = hits(extra)
        one = one_hot(hit)
        by_key = jnp.where(hit, extra[0:1], f32(0.0)).astype(bf16)
        by_value = jnp.where(hit, extra[1:2], f32(0.0)).astype(bf16)
        kp[row] = jnp.dot(one, recv[row, pl.ds(0, tok)], preferred_element_type=f32)
        vp[row] = jnp.dot(one, recv[row, pl.ds(tok, tok)], preferred_element_type=f32)
        xp[row] = jnp.dot(by_key, low, preferred_element_type=f32) + jnp.dot(
            by_value, high, preferred_element_type=f32
        )

    def place_query(turn, other):
        qp[turn] = jnp.dot(
            one_hot(hits(aux_of(2 * other + core))), recv_q[other], preferred_element_type=f32
        )

    place(mine)
    own_aux().wait_recv()
    own_forward().wait_recv()
    place(2 * chip + 1 - core)

    def of_turn(t):
        return t

    @pl.loop(1, chips)
    def _(t):
        d = of_turn(t)
        out_aux(d).wait_recv()
        forward_aux(d).start()
        outgoing(d).wait_recv()
        forward(d).start()
        place(2 * (chip ^ d) + core)

        @pl.when(t > 1)
        def _():
            before = of_turn(t - 1)
            forward_aux(before).wait_recv()
            forward(before).wait_recv()
            place(2 * (chip ^ before) + 1 - core)

    last = turns[-1]
    forward_aux(last).wait_recv()
    forward(last).wait_recv()
    place(2 * (chip ^ last) + 1 - core)

    sel_lane = lax.broadcasted_iota(jnp.int32, (16, width), 1)
    sel_row = lax.broadcasted_iota(jnp.int32, (16, width), 0)
    select = (sel_lane == jnp.where(sel_row < 8, 0, width // 2)).astype(f32).astype(bf16)
    factor = width ** (-0.5)
    keys_here = vis_ref.shape[1]
    chunk_rows = CHUNK * 8
    nt = (((1,), (1,)), ((), ()))

    def rows_of(t):
        return pl.ds(pl.multiple_of(t * 8, 8), 8)

    @pl.loop(0, slots // 8 // UNROLL)
    def _(at_group):
        for u in range(UNROLL):
            t = at_group * UNROLL + u
            rows = rows_of(t)
            kb[t] = kp[:, rows, :].reshape(keys_here, width).astype(bf16)
            vb[t] = vp[:, rows, :].reshape(keys_here, width).astype(bf16)
            extra = xp[:, rows, :].reshape(keys_here, width).astype(bf16)
            scales[t] = lax.dot_general(select, extra, nt, preferred_element_type=f32)

    def attend_groups(base, groups):
        here = pl.ds(base, CHUNK)
        allowed = vis_ref[pl.ds(base * 8, chunk_rows), :]
        scale = [scales[t] for t in groups]
        query = [qp[here, rows_of(t), :].reshape(chunk_rows, width).astype(bf16) for t in groups]
        scores = [
            lax.dot_general(q, kb[t], nt, preferred_element_type=f32)
            for q, t in zip(query, groups)
        ]
        visible = [allowed * c[0:1] > 0 for c in scale]
        scores = [
            jnp.where(ok, s * (c[0:1] * factor), f32(-1e30))
            for ok, s, c in zip(visible, scores, scale)
        ]
        highest = [jnp.max(s, axis=1, keepdims=True) for s in scores]
        unnormed = [
            jnp.where(ok, jnp.exp(s - m), f32(0.0))
            for ok, s, m in zip(visible, scores, highest)
        ]
        weights = [(e * c[8:9]).astype(bf16) for e, c in zip(unnormed, scale)]
        numerator = [
            jnp.dot(w, vb[t], preferred_element_type=f32) for w, t in zip(weights, groups)
        ]
        denominator = [jnp.sum(e, axis=1, keepdims=True) for e in unnormed]
        safe = [jnp.where(n > 0, n, f32(1.0)) for n in denominator]
        result = [(n / d).astype(bf16).astype(f32) for n, d in zip(numerator, safe)]
        for r, t in zip(result, groups):
            op[here, rows_of(t), :] = r.reshape(CHUNK, 8, width)

    eye = (
        lax.broadcasted_iota(jnp.int32, (tok, tok), 0)
        == lax.broadcasted_iota(jnp.int32, (tok, tok), 1)
    ).astype(f32).astype(bf16)

    def answer(turn, other):
        columns = lax.dot_general(
            eye, recv_aux[2 * other + core], (((1,), (1,)), ((), ())), preferred_element_type=f32,
        )
        slot = (columns[:, 2:3] + columns[:, 3:4]).astype(jnp.int32)
        hit = lax.broadcasted_iota(jnp.int32, (tok, slots), 1) == slot
        return jnp.dot(
            one_hot(hit), op[turn].astype(bf16), preferred_element_type=f32
        ).astype(bf16)

    def reply(d):
        other = chip ^ d
        return copy(ans.at[other], back.at[chip], bsend.at[d], brecv.at[d], at(other))

    place_query(0, chip)
    for part in range(chips // CHUNK):
        first_turn = part * CHUNK
        start = max(first_turn, 1)

        @pl.loop(start, first_turn + CHUNK)
        def _(t):
            d = of_turn(t)
            outgoing_query(d).wait_recv()
            place_query(t, chip ^ d)

        @pl.loop(0, slots // 8 // UNROLL)
        def _(at_group):
            attend_groups(first_turn, [at_group * UNROLL + u for u in range(UNROLL)])

        @pl.loop(start, first_turn + CHUNK)
        def _(t):
            other = chip ^ of_turn(t)
            ans[other] = answer(t, other)

            @pl.when(t > start)
            def _():
                reply(of_turn(t - 1)).start()

        reply(of_turn(first_turn + CHUNK - 1)).start()

    back[chip] = answer(0, chip)
    own_forward().wait_send()
    own_aux().wait_send()

    @pl.loop(1, chips)
    def _(d):
        out_aux(d).wait_send()
        outgoing(d).wait_send()
        outgoing_query(d).wait_send()
        forward_aux(d).wait_send()
        forward(d).wait_send()
        reply(d).wait()

    out_ref[...] = jnp.swapaxes(back[...], 0, 1)


def by_head(queries, key_rows, value_rows, key_scale, value_scale, cluster_label):
    tok, heads, width = queries.shape
    half = lax.axis_size("inner") // 2
    chips = lax.axis_size("outer") * half
    clusters = COARSE * FINE
    slots = clusters * max(2, 2 * tok // clusters)
    vm = pl.BlockSpec(memory_space=pltpu.VMEM)
    anywhere = pl.BlockSpec(memory_space=pl.ANY)
    dma = pltpu.SemaphoreType.DMA
    f32, bf16 = jnp.float32, jnp.bfloat16
    return pl.pallas_call(
        lambda *refs: exchange_kernel(chips, half, tok, slots, *refs),
        out_shape=jax.ShapeDtypeStruct((tok, heads, width), bf16),
        in_specs=[anywhere] * 3 + [vm] * 3,
        out_specs=vm,
        scratch_shapes=[
            pltpu.VMEM((3, tok, heads, width), bf16),
            pltpu.VMEM((heads, 2 * tok, width), bf16),
            pltpu.VMEM((heads, tok, width), bf16),
            pltpu.VMEM((heads, AUX, tok), bf16),
            pltpu.VMEM((2 * chips, 2 * tok, width), bf16),
            pltpu.VMEM((chips, tok, width), bf16),
            pltpu.VMEM((2 * chips, AUX, tok), bf16),
            pltpu.VMEM((chips, tok, width), bf16),
            pltpu.VMEM((chips, tok, width), bf16),
            pltpu.VMEM((2 * chips, slots, width), f32),
            pltpu.VMEM((2 * chips, slots, width), f32),
            pltpu.VMEM((2 * chips, slots, width), f32),
            pltpu.VMEM((chips, slots, width), f32),
            pltpu.VMEM((chips, slots, width), f32),
            pltpu.VMEM((slots // 8, 16 * chips, width), bf16),
            pltpu.VMEM((slots // 8, 16 * chips, width), bf16),
            pltpu.VMEM((slots // 8, 16, 16 * chips), f32),
            pltpu.VMEM((8 * chips, 16 * chips), f32),
            pltpu.VMEM((2, heads, tok), f32),
            dma((3,)),
        ]
        + [dma((chips,))] * 12,
        compiler_params=pltpu.CompilerParams(
            collective_id=0, has_side_effects=True, vmem_limit_bytes=63 * 1024 * 1024
        ),
        name="clustered",
    )(
        key_rows, value_rows, queries, key_scale.T, value_scale.T, cluster_label.swapaxes(1, 2)
    )


UNROLL = 16
CHUNK = 4


def route(queries, key_rows, value_rows, key_scale, value_scale, cluster_label):
    tok, heads, width = queries.shape
    devices = lax.axis_size("outer") * lax.axis_size("inner")
    even = lax.axis_size("inner") % 2 == 0 and tok == 2 * width
    even = even and heads & (heads - 1) == 0 and heads % CHUNK == 0
    if devices == 2 * heads and even and 2 * tok == 4 * COARSE * FINE:
        return by_head(queries, key_rows, value_rows, key_scale, value_scale, cluster_label)
    return shards(queries, key_rows, value_rows, key_scale, value_scale, cluster_label)


def solution(mesh):
    placed = (
        P(("outer", "inner"), None, None),
        P(("outer", "inner"), None, None),
        P(("outer", "inner"), None, None),
        P(("outer", "inner"), None),
        P(("outer", "inner"), None),
        P(None, ("outer", "inner"), None),
    )
    return jax.shard_map(
        route,
        mesh=mesh,
        in_specs=placed,
        out_specs=P(("outer", "inner"), None, None),
        check_vma=False,
    )
```
